32 devices in a mesh: grp: 2 (over x), blk: 16 (over z, y, core).
Axes of the slice: x: 2, y: 2, z: 4, core: 2. Of those that a mesh axis runs over, the one named last changes fastest.
Arguments:
- params: bfloat16 [2, 7168, 4096], P('grp', 'blk'), may hold values from -0.0625 to 0.0625
- tracker: bfloat16 [2, 7168, 4096], P('grp', 'blk'), may hold values from -0.29882812 to 0.29882812
- hidden: bfloat16 [256, 7168], P('grp', 'blk'), may hold values from -6 to 6
- target: bfloat16 [256, 4096], P('grp'), may hold values from -6 to 6
Outputs:
- params_next: bfloat16 [2, 7168, 4096], P('grp', 'blk')
- tracker_next: bfloat16 [2, 7168, 4096], P('grp', 'blk')
The draws below stay inside these ranges and needn't reach their ends.
All inputs are finite; a program needn't handle non-finite values.
Results may differ from the reference program's by a relative error of at most 0.01.
Values may be sent and summed in bfloat16 or wider, within the bound.
A program may use at most 192 MiB of HBM per device.

```python
import jax
import jax.numpy as jnp
from jax import lax

D = 4096
FF_WIN = 7168
TOK = 128
ALL_TOK = 256
N_GRP = 2


def levels(rng, extent, split, smallest, largest):
    def one(position, parts):
        draws = jax.random.uniform(jax.random.fold_in(jax.random.fold_in(rng, 6), position), (parts,), jnp.float32, smallest / len(split), largest / len(split))
        return jnp.repeat(jnp.exp(draws), extent[position] // parts).reshape((-1,) + (1,) * (len(extent) - position - 1))

    loudness = one(*split[0])
    for cut in split[1:]:
        loudness = loudness * one(*cut)
    return loudness


def noise(key, shape, width, bound, split=(), dtype=jnp.bfloat16):
    gain = levels(key, shape, split, -0.22, 0.18) if split else 1.0
    entries = jax.random.normal(key, shape, jnp.float32) * width * gain
    return jnp.minimum(jnp.maximum(entries, -bound), bound).astype(dtype)


def setup_inputs(seed: int = 0) -> dict:
    key_of = jax.random.split(jax.random.key(seed), 5)
    return {
        "params": noise(key_of[0], (N_GRP, FF_WIN, D), FF_WIN ** -0.5, 0.0625, ((0, 2), (1, 16))),
        "tracker": noise(key_of[1], (N_GRP, FF_WIN, D), 0.05, 0.29882812, ((0, 2), (1, 16))),
        "hidden": noise(key_of[2], (ALL_TOK, FF_WIN), 1.0, 6.0, ((0, 2), (1, 16))),
        "target": noise(key_of[3], (ALL_TOK, D), 1.0, 6.0, ((0, 2),)),
    }


step_size = 0.05


def mix(value):
    count = value.shape[0]
    zero_row = jnp.zeros_like(value[:1])
    left = jnp.concatenate([zero_row, value[:-1]], 0)
    right = jnp.concatenate([value[1:], zero_row], 0)
    place = jnp.arange(count)
    has_left = (place > 0).astype(jnp.float32)[:, None, None]
    has_right = (place < count - 1).astype(jnp.float32)[:, None, None]
    return value + has_left * (left - value) / 3.0 + has_right * (right - value) / 3.0


def gradient(weights, hidden_rows, target_rows):
    output = jnp.dot(hidden_rows, weights, preferred_element_type=jnp.float32)
    resid = jnp.tanh(output - target_rows.astype(jnp.float32)).astype(jnp.bfloat16)
    total = lax.dot_general(hidden_rows, resid, (((0,), (0,)), ((), ())), preferred_element_type=jnp.float32)
    return total / TOK


def reference(params, tracker, hidden, target):
    groups = params.shape[0]
    olds = []
    for replica in range(groups):
        olds.append(gradient(params[replica], hidden[replica * TOK:(replica + 1) * TOK], target[replica * TOK:(replica + 1) * TOK]))
    params_next = (mix(mix(params.astype(jnp.float32))) - step_size * tracker.astype(jnp.float32)).astype(jnp.bfloat16)
    mixed_tracker = mix(mix(tracker.astype(jnp.float32)))
    outcome = []
    for replica in range(groups):
        fresh = gradient(params_next[replica], hidden[replica * TOK:(replica + 1) * TOK], target[replica * TOK:(replica + 1) * TOK])
        outcome.append(mixed_tracker[replica] + fresh - olds[replica])
    tracker_next = jnp.stack(outcome).astype(jnp.bfloat16)
    return params_next, tracker_next
```

```python
import functools

import jax
import jax.numpy as jnp
from jax import lax
from jax.experimental import pallas as pl
from jax.experimental.pallas import tpu as pltpu
from jax.sharding import PartitionSpec as P

step_size = 0.05
MESH = pl.DeviceIdType.MESH


def mix_weights(position, groups):
    def has(spot):
        return ((spot >= 0) & (spot < groups)).astype(jnp.float32)

    def row(spot):
        a, b = has(spot - 1) / 3.0, has(spot + 1) / 3.0
        return a, 1.0 - a - b, b

    here, before, after = row(position), row(position - 1), row(position + 1)
    return {
        -2: here[0] * before[0],
        -1: here[0] * before[1] + here[1] * here[0],
        0: here[1] * here[1] + here[0] * before[2] + here[2] * after[0],
        1: here[2] * after[1] + here[1] * here[2],
        2: here[2] * after[2],
    }


def exchange(value, groups):
    if groups == 2:
        return {(-1, 1): lax.ppermute(value, "grp", [(0, 1), (1, 0)])}
    received = {}
    for offset in (-2, -1, 1, 2):
        pairs = [(i, i - offset) for i in range(groups) if 0 <= i - offset < groups]
        if pairs:
            received[(offset,)] = lax.ppermute(value, "grp", pairs)
    return received


def mixed(own, others, weights):
    total = weights[0] * own.astype(jnp.float32)
    for offsets, value in others.items():
        total = total + sum(weights[o] for o in offsets) * value.astype(jnp.float32)
    return total


PIECES = 4


def residual_kernel(
    z_size, part_ref, target_ref, out_ref, core_in, core_sum, y_in, y_sum, z_in, *sems
):
    (core_s, core_r, y_s, y_r, z_s, z_r, gz_s, gz_r, gy_s, gy_r, gc_s, gc_r) = sems
    me = lax.axis_index("blk")
    c = lax.rem(me, 2)
    y = lax.rem(lax.div(me, 2), 2)
    z = lax.div(me, 4)
    core_peer = z * 4 + y * 2 + (1 - c)
    y_peer = z * 4 + (1 - y) * 2 + c
    z_spots = [lax.rem(z + k, z_size) for k in range(1, z_size)]
    z_peers = [spot * 4 + y * 2 + c for spot in z_spots]
    width = target_ref.shape[-1] // PIECES
    columns = [pl.ds(q * width, width) for q in range(PIECES)]

    barrier = pltpu.get_barrier_semaphore()
    for peer in [core_peer, y_peer, *z_peers]:
        pl.semaphore_signal(barrier, inc=1, device_id={"blk": peer}, device_id_type=MESH)
    pl.semaphore_wait(barrier, z_size + 1)

    def send(src, dst, send_sem, recv_sem, peer):
        copy = pltpu.make_async_remote_copy(
            src_ref=src,
            dst_ref=dst,
            send_sem=send_sem,
            recv_sem=recv_sem,
            device_id={"blk": peer},
            device_id_type=MESH,
        )
        copy.start()
        return copy

    over_core = [
        send(part_ref.at[:, :, 1 - c, :, at], core_in.at[:, :, :, at], core_s.at[q], core_r.at[q], core_peer)
        for q, at in enumerate(columns)
    ]
    over_y = []
    for q, at in enumerate(columns):
        over_core[q].wait_recv()
        core_sum[:, :, :, at] = part_ref[:, :, c, :, at] + core_in[:, :, :, at]
        over_y.append(
            send(core_sum.at[:, 1 - y, :, at], y_in.at[:, :, at], y_s.at[q], y_r.at[q], y_peer)
        )
    over_z = []
    for q, at in enumerate(columns):
        over_y[q].wait_recv()
        y_sum[:, :, at] = core_sum[:, y, :, at] + y_in[:, :, at]
        over_z.append([
            send(y_sum.at[spot, :, at], z_in.at[k, :, at], z_s.at[q, k], z_r.at[q, k], z_peers[k])
            for k, spot in enumerate(z_spots)
        ])
    give_z = []
    for q, at in enumerate(columns):
        total = y_sum[z, :, at] - target_ref[:, at].astype(jnp.float32)
        for k, copy in enumerate(over_z[q]):
            copy.wait_recv()
            total = total + z_in[k, :, at]
        out_ref[z, y, c, :, at] = jnp.tanh(total).astype(jnp.bfloat16)
        mine = out_ref.at[z, y, c, :, at]
        give_z.append([
            send(mine, mine, gz_s.at[q, k], gz_r.at[q, k], peer) for k, peer in enumerate(z_peers)
        ])
    give_y = []
    for q, at in enumerate(columns):
        for copy in give_z[q]:
            copy.wait_recv()
        mine = out_ref.at[:, y, c, :, at]
        give_y.append(send(mine, mine, gy_s.at[q], gy_r.at[q], y_peer))
    give_core = []
    for q, at in enumerate(columns):
        give_y[q].wait_recv()
        mine = out_ref.at[:, :, c, :, at]
        give_core.append(send(mine, mine, gc_s.at[q], gc_r.at[q], core_peer))
    for copy in give_core:
        copy.wait_recv()
    for copy in [*over_core, *over_y, *sum(over_z, []), *sum(give_z, []), *give_y, *give_core]:
        copy.wait_send()


def residual(output, own_target, n, which):
    tokens, width = output.shape
    share, z_size = tokens // n, n // 4
    one = pltpu.SemaphoreType.DMA((PIECES,))
    many = pltpu.SemaphoreType.DMA((PIECES, z_size - 1))
    resid = pl.pallas_call(
        functools.partial(residual_kernel, z_size),
        out_shape=jax.ShapeDtypeStruct((z_size, 2, 2, share, width), jnp.bfloat16),
        in_specs=[pl.BlockSpec(memory_space=pltpu.VMEM)] * 2,
        out_specs=pl.BlockSpec(memory_space=pltpu.VMEM),
        scratch_shapes=[
            pltpu.VMEM((z_size, 2, share, width), jnp.float32),
            pltpu.VMEM((z_size, 2, share, width), jnp.float32),
            pltpu.VMEM((z_size, share, width), jnp.float32),
            pltpu.VMEM((z_size, share, width), jnp.float32),
            pltpu.VMEM((z_size - 1, share, width), jnp.float32),
            one, one, one, one, many, many, many, many, one, one, one, one,
        ],
        compiler_params=pltpu.CompilerParams(collective_id=which, has_side_effects=True),
        cost_estimate=pl.CostEstimate(flops=0, bytes_accessed=100 * tokens * width, transcendentals=0),
        name="residual",
    )(output.reshape(z_size, 2, 2, share, width), own_target)
    return resid.reshape(tokens, width)


def add_kernel(count, weights_ref, base_ref, *refs):
    out_ref = refs[-1]
    total = base_ref[...]
    for i, other in enumerate(refs[:count]):
        total = total + weights_ref[i] * other[...].astype(jnp.float32)
    out_ref[...] = total.astype(out_ref.dtype)


def add_others(base, others, weights, block):
    rows, width = base.shape
    count = others[0].shape[0] // block
    here = pl.BlockSpec((block, width), lambda i: (i, 0))
    return pl.pallas_call(
        functools.partial(add_kernel, len(others)),
        grid=(count,),
        out_shape=jax.ShapeDtypeStruct((rows, width), jnp.bfloat16),
        in_specs=[pl.BlockSpec(memory_space=pltpu.SMEM), here] + [here] * len(others),
        out_specs=here,
        compiler_params=pltpu.CompilerParams(dimension_semantics=("arbitrary",)),
        cost_estimate=pl.CostEstimate(
            flops=4 * count * block * width, bytes_accessed=8 * count * block * width, transcendentals=0
        ),
        name="add_others",
    )(weights, base, *others)


def body(params, tracker, hidden, target):
    groups, n = lax.axis_size("grp"), lax.axis_size("blk")
    weights = mix_weights(lax.axis_index("grp"), groups)
    tokens = hidden.shape[0]
    share = tokens // n
    own_target = lax.dynamic_slice_in_dim(target, lax.axis_index("blk") * share, share, 0)
    params, tracker = params[0], tracker[0]
    rows = params.shape[0]
    block = 16
    first = rows * 5 // 7 // 16 * 16
    ends = sorted({first, max(first, rows - 32), max(first, rows - 8), rows})
    cuts = list(zip([0, *ends[:-1]], ends))
    other_params = exchange(params, groups)
    other_tracker = [exchange(tracker[lo:hi], groups) for lo, hi in cuts]
    output_old = jnp.dot(hidden, params, preferred_element_type=jnp.float32)
    resid_old = residual(output_old, own_target, n, 0)
    params_next = (
        mixed(params, other_params, weights) - step_size * tracker.astype(jnp.float32)
    ).astype(jnp.bfloat16)
    output_new = jnp.dot(hidden, params_next, preferred_element_type=jnp.float32)
    resid_new = residual(output_new, own_target, n, 1)
    change = lax.dot_general(
        jnp.concatenate([hidden, -hidden], 0),
        jnp.concatenate([resid_new, resid_old], 0),
        (((0,), (0,)), ((), ())),
        preferred_element_type=jnp.float32,
    )
    base = weights[0] * tracker.astype(jnp.float32) + change / tokens
    late = lax.optimization_barrier([base[lo:hi] for lo, hi in cuts[1:]])
    gains = jnp.stack([sum(weights[o] for o in offsets) for offsets in other_tracker[0]])
    early = list(other_tracker[0].values())
    step = next(size for size in (10 * block, 4 * block, block) if first % size == 0)
    tracker_next = add_others(base, early, gains, step)
    for (lo, _), piece, received in zip(cuts[1:], late, other_tracker[1:]):
        for gain, value in zip(gains, received.values()):
            piece = piece + gain * value.astype(jnp.float32)
        tracker_next = lax.dynamic_update_slice(tracker_next, piece.astype(jnp.bfloat16), (lo, 0))
    return (params_next[None], tracker_next[None])


def solution(mesh):
    placed = (P("grp", "blk", None), P("grp", "blk", None), P("grp", "blk"), P("grp", None))
    return jax.shard_map(
        body,
        mesh=mesh,
        in_specs=placed,
        out_specs=(P("grp", "blk", None), P("grp", "blk", None)),
        check_vma=False,
    )
```

```python
import functools

import jax
import jax.numpy as jnp
from jax import lax
from jax.experimental import pallas as pl
from jax.experimental.pallas import tpu as pltpu
from jax.sharding import PartitionSpec as P


step_size = 0.05
MESH = pl.DeviceIdType.MESH


def mix_weights(position, groups):
    def has(spot):
        return ((spot >= 0) & (spot < groups)).astype(jnp.float32)

    def row(spot):
        a, b = has(spot - 1) / 3.0, has(spot + 1) / 3.0
        return a, 1.0 - a - b, b

    here, before, after = row(position), row(position - 1), row(position + 1)
    return {
        -2: here[0] * before[0],
        -1: here[0] * before[1] + here[1] * here[0],
        0: here[1] * here[1] + here[0] * before[2] + here[2] * after[0],
        1: here[2] * after[1] + here[1] * here[2],
        2: here[2] * after[2],
    }


def exchange(value, groups):
    if groups == 2:
        return {(-1, 1): lax.ppermute(value, "grp", [(0, 1), (1, 0)])}
    received = {}
    for offset in (-2, -1, 1, 2):
        pairs = [(i, i - offset) for i in range(groups) if 0 <= i - offset < groups]
        if pairs:
            received[(offset,)] = lax.ppermute(value, "grp", pairs)
    return received


def exchange_uneven(value, groups, n):
    if groups != 2 or n % 2:
        return exchange(value, groups)
    both = ("grp", "blk")
    sides = [(g, b) for g in range(groups) for b in range(0, n, 2)]
    lent = lax.ppermute(value, both, [(g * n + b, g * n + b + 1) for g, b in sides])
    for_even = lax.ppermute(lent, both, [(g * n + b + 1, (1 - g) * n + b) for g, b in sides])
    for_odd = lax.ppermute(value, both, [(g * n + b + 1, (1 - g) * n + b + 1) for g, b in sides])
    return {(-1, 1): for_even + for_odd}


def mixed(own, others, weights):
    total = weights[0] * own.astype(jnp.float32)
    for offsets, value in others.items():
        total = total + sum(weights[o] for o in offsets) * value.astype(jnp.float32)
    return total


PIECES = 4


def residual_kernel(
    z_size, part_ref, target_ref, out_ref, core_in, core_sum, y_in, y_sum, z_in, *sems
):
    (core_s, core_r, y_s, y_r, z_s, z_r, gz_s, gz_r, gy_s, gy_r, gc_s, gc_r) = sems
    me = lax.axis_index("blk")
    c = lax.rem(me, 2)
    y = lax.rem(lax.div(me, 2), 2)
    z = lax.div(me, 4)
    core_peer = z * 4 + y * 2 + (1 - c)
    y_peer = z * 4 + (1 - y) * 2 + c
    z_spots = [lax.rem(z + k, z_size) for k in range(1, z_size)]
    z_peers = [spot * 4 + y * 2 + c for spot in z_spots]
    width = target_ref.shape[-1] // PIECES
    columns = [pl.ds(q * width, width) for q in range(PIECES)]

    barrier = pltpu.get_barrier_semaphore()
    for peer in [core_peer, y_peer, *z_peers]:
        pl.semaphore_signal(barrier, inc=1, device_id={"blk": peer}, device_id_type=MESH)
    pl.semaphore_wait(barrier, z_size + 1)

    def send(src, dst, send_sem, recv_sem, peer):
        copy = pltpu.make_async_remote_copy(
            src_ref=src,
            dst_ref=dst,
            send_sem=send_sem,
            recv_sem=recv_sem,
            device_id={"blk": peer},
            device_id_type=MESH,
        )
        copy.start()
        return copy

    over_core = [
        send(part_ref.at[:, :, 1 - c, :, at], core_in.at[:, :, :, at], core_s.at[q], core_r.at[q], core_peer)
        for q, at in enumerate(columns)
    ]
    over_y = []
    for q, at in enumerate(columns):
        over_core[q].wait_recv()
        core_sum[:, :, :, at] = part_ref[:, :, c, :, at] + core_in[:, :, :, at]
        over_y.append(
            send(core_sum.at[:, 1 - y, :, at], y_in.at[:, :, at], y_s.at[q], y_r.at[q], y_peer)
        )
    over_z = []
    for q, at in enumerate(columns):
        over_y[q].wait_recv()
        y_sum[:, :, at] = core_sum[:, y, :, at] + y_in[:, :, at]
        over_z.append([
            send(y_sum.at[spot, :, at], z_in.at[k, :, at], z_s.at[q, k], z_r.at[q, k], z_peers[k])
            for k, spot in enumerate(z_spots)
        ])
    give_z = []
    for q, at in enumerate(columns):
        total = y_sum[z, :, at] - target_ref[:, at].astype(jnp.float32)
        for k, copy in enumerate(over_z[q]):
            copy.wait_recv()
            total = total + z_in[k, :, at]
        out_ref[z, y, c, :, at] = jnp.tanh(total).astype(jnp.bfloat16)
        mine = out_ref.at[z, y, c, :, at]
        give_z.append([
            send(mine, mine, gz_s.at[q, k], gz_r.at[q, k], peer) for k, peer in enumerate(z_peers)
        ])
    give_y = []
    for q, at in enumerate(columns):
        for copy in give_z[q]:
            copy.wait_recv()
        mine = out_ref.at[:, y, c, :, at]
        give_y.append(send(mine, mine, gy_s.at[q], gy_r.at[q], y_peer))
    give_core = []
    for q, at in enumerate(columns):
        give_y[q].wait_recv()
        mine = out_ref.at[:, :, c, :, at]
        give_core.append(send(mine, mine, gc_s.at[q], gc_r.at[q], core_peer))
    for copy in give_core:
        copy.wait_recv()
    for copy in [*over_core, *over_y, *sum(over_z, []), *sum(give_z, []), *give_y, *give_core]:
        copy.wait_send()


def residual(output, own_target, n, which):
    tokens, width = output.shape
    share, z_size = tokens // n, n // 4
    one = pltpu.SemaphoreType.DMA((PIECES,))
    many = pltpu.SemaphoreType.DMA((PIECES, z_size - 1))
    resid = pl.pallas_call(
        functools.partial(residual_kernel, z_size),
        out_shape=jax.ShapeDtypeStruct((z_size, 2, 2, share, width), jnp.bfloat16),
        in_specs=[pl.BlockSpec(memory_space=pltpu.VMEM)] * 2,
        out_specs=pl.BlockSpec(memory_space=pltpu.VMEM),
        scratch_shapes=[
            pltpu.VMEM((z_size, 2, share, width), jnp.float32),
            pltpu.VMEM((z_size, 2, share, width), jnp.float32),
            pltpu.VMEM((z_size, share, width), jnp.float32),
            pltpu.VMEM((z_size, share, width), jnp.float32),
            pltpu.VMEM((z_size - 1, share, width), jnp.float32),
            one, one, one, one, many, many, many, many, one, one, one, one,
        ],
        compiler_params=pltpu.CompilerParams(collective_id=which, has_side_effects=True),
        cost_estimate=pl.CostEstimate(flops=0, bytes_accessed=100 * tokens * width, transcendentals=0),
        name="residual",
    )(output.reshape(z_size, 2, 2, share, width), own_target)
    return resid.reshape(tokens, width)


def add_kernel(count, weights_ref, base_ref, *refs):
    out_ref = refs[-1]
    total = base_ref[...]
    for i, other in enumerate(refs[:count]):
        total = total + weights_ref[i] * other[...].astype(jnp.float32)
    out_ref[...] = total.astype(out_ref.dtype)


def add_others(base, others, weights, block):
    rows, width = base.shape
    count = others[0].shape[0] // block
    here = pl.BlockSpec((block, width), lambda i: (i, 0))
    return pl.pallas_call(
        functools.partial(add_kernel, len(others)),
        grid=(count,),
        out_shape=jax.ShapeDtypeStruct((rows, width), jnp.bfloat16),
        in_specs=[pl.BlockSpec(memory_space=pltpu.SMEM), here] + [here] * len(others),
        out_specs=here,
        compiler_params=pltpu.CompilerParams(dimension_semantics=("arbitrary",)),
        cost_estimate=pl.CostEstimate(
            flops=4 * count * block * width, bytes_accessed=8 * count * block * width, transcendentals=0
        ),
        name="add_others",
    )(weights, base, *others)


def step(params, tracker, hidden, target):
    groups, n = lax.axis_size("grp"), lax.axis_size("blk")
    weights = mix_weights(lax.axis_index("grp"), groups)
    tokens = hidden.shape[0]
    share = tokens // n
    own_target = lax.dynamic_slice_in_dim(target, lax.axis_index("blk") * share, share, 0)
    params, tracker = params[0], tracker[0]
    rows = params.shape[0]
    block = 16
    first = rows * 5 // 7 // 16 * 16
    ends = sorted({first, max(first, rows - 32), max(first, rows - 8), rows})
    cuts = list(zip([0, *ends[:-1]], ends))
    other_params = exchange(params, groups)
    slices = [tracker[lo:hi] for lo, hi in cuts]
    other_tracker = []
    for piece in slices[:-1]:
        other_tracker.append(exchange(piece, groups))
    other_tracker.append(exchange_uneven(slices[-1], groups, n))
    output_old = jnp.dot(hidden, params, preferred_element_type=jnp.float32)
    resid_old = residual(output_old, own_target, n, 0)
    params_next = (
        mixed(params, other_params, weights) - step_size * tracker.astype(jnp.float32)
    ).astype(jnp.bfloat16)
    output_new = jnp.dot(hidden, params_next, preferred_element_type=jnp.float32)
    resid_new = residual(output_new, own_target, n, 1)
    change = lax.dot_general(
        jnp.concatenate([hidden, -hidden], 0),
        jnp.concatenate([resid_new, resid_old], 0),
        (((0,), (0,)), ((), ())),
        preferred_element_type=jnp.float32,
    )
    base = weights[0] * tracker.astype(jnp.float32) + change / tokens
    late = lax.optimization_barrier([base[lo:hi] for lo, hi in cuts[1:]])
    gains = jnp.stack([sum(weights[o] for o in offsets) for offsets in other_tracker[0]])
    early = list(other_tracker[0].values())
    height = next(size for size in (10 * block, 4 * block, block) if first % size == 0)
    tracker_next = add_others(base, early, gains, height)
    for (lo, _), piece, received in zip(cuts[1:], late, other_tracker[1:]):
        for gain, value in zip(gains, received.values()):
            piece = piece + gain * value.astype(jnp.float32)
        tracker_next = lax.dynamic_update_slice(tracker_next, piece.astype(jnp.bfloat16), (lo, 0))
    return (params_next[None], tracker_next[None])


def solution(mesh):
    placed = (P("grp", "blk", None), P("grp", "blk", None), P("grp", "blk"), P("grp", None))
    return jax.shard_map(
        step,
        mesh=mesh,
        in_specs=placed,
        out_specs=(P("grp", "blk", None), P("grp", "blk", None)),
        check_vma=False,
    )
```

```python
import functools

import jax
import jax.numpy as jnp
from jax import lax
from jax.experimental import pallas as pl
from jax.experimental.pallas import tpu as pltpu
from jax.sharding import PartitionSpec as P


step_size = 0.05
MESH = pl.DeviceIdType.MESH


def mix_weights(position, groups):
    def has(spot):
        return ((spot >= 0) & (spot < groups)).astype(jnp.float32)

    def row(spot):
        a, b = has(spot - 1) / 3.0, has(spot + 1) / 3.0
        return a, 1.0 - a - b, b

    here, before, after = row(position), row(position - 1), row(position + 1)
    return {
        -2: here[0] * before[0],
        -1: here[0] * before[1] + here[1] * here[0],
        0: here[1] * here[1] + here[0] * before[2] + here[2] * after[0],
        1: here[2] * after[1] + here[1] * here[2],
        2: here[2] * after[2],
    }


def exchange(value, groups):
    if groups == 2:
        return {(-1, 1): lax.ppermute(value, "grp", [(0, 1), (1, 0)])}
    received = {}
    for offset in (-2, -1, 1, 2):
        pairs = [(i, i - offset) for i in range(groups) if 0 <= i - offset < groups]
        if pairs:
            received[(offset,)] = lax.ppermute(value, "grp", pairs)
    return received


def helpers(z_size):
    return [3] + [4 * z + 1 for z in range(1, z_size)]


def mixed(own, others, weights):
    total = weights[0] * own.astype(jnp.float32)
    for offsets, value in others.items():
        total = total + sum(weights[o] for o in offsets) * value.astype(jnp.float32)
    return total


PIECES = 4


def residual_kernel(z_size, lends, part_ref, target_ref, *refs):
    if lends is not None:
        near_ref, out_ref, far_ref, *refs = refs
    else:
        out_ref, *refs = refs
    core_in, core_sum, y_in, y_sum, z_in, *sems = refs
    (core_s, core_r, y_s, y_r, z_s, z_r, gz_s, gz_r, gy_s, gy_r, gc_s, gc_r) = sems[:12]
    me = lax.axis_index("blk")
    c = lax.rem(me, 2)
    y = lax.rem(lax.div(me, 2), 2)
    z = lax.div(me, 4)
    core_peer = z * 4 + y * 2 + (1 - c)
    y_peer = z * 4 + (1 - y) * 2 + c
    z_spots = [lax.rem(z + k, z_size) for k in range(1, z_size)]
    z_peers = [spot * 4 + y * 2 + c for spot in z_spots]
    width = target_ref.shape[-1] // PIECES
    columns = [pl.ds(q * width, width) for q in range(PIECES)]

    greeted = [core_peer, y_peer, *z_peers]
    if lends is not None:
        relay_s, relay_r = sems[12:]
        greeted += [z * 4 + (1 - y) * 2 + 1 - c, *[spot * 4 + y * 2 + 1 - c for spot in z_spots]]
        home = (lax.axis_index("grp") == (1 if lends else 0)) & (me == 0)
        helps = [
            (lax.axis_index("grp") == (1 if lends else 0)) & (me == spot) for spot in helpers(z_size)
        ]
        receives = functools.reduce(lambda a, b: a | b, helps) if lends else home

        @pl.when(jnp.logical_not(receives))
        def _():
            far_ref[...] = jnp.zeros_like(far_ref)

    barrier = pltpu.get_barrier_semaphore()
    for peer in greeted:
        pl.semaphore_signal(barrier, inc=1, device_id={"blk": peer}, device_id_type=MESH)
    pl.semaphore_wait(barrier, len(greeted))

    def relay(j):
        length = target_ref.shape[-1] // z_size
        at = pl.ds(j * length, length)
        return pltpu.make_async_remote_copy(
            src_ref=near_ref.at[:, at] if lends else near_ref,
            dst_ref=far_ref if lends else far_ref.at[:, at],
            send_sem=relay_s.at[j],
            recv_sem=relay_r.at[j],
            device_id={"blk": helpers(z_size)[j] if lends else 0},
            device_id_type=MESH,
        )

    def relay_all(act):
        for j in range(z_size):
            pl.when(home if lends else helps[j])(functools.partial(act, j))

    if lends is not None:
        relay_all(lambda j: relay(j).start())

    def send(src, dst, send_sem, recv_sem, peer):
        copy = pltpu.make_async_remote_copy(
            src_ref=src,
            dst_ref=dst,
            send_sem=send_sem,
            recv_sem=recv_sem,
            device_id={"blk": peer},
            device_id_type=MESH,
        )
        copy.start()
        return copy

    over_core = [
        send(part_ref.at[:, :, 1 - c, :, at], core_in.at[:, :, :, at], core_s.at[q], core_r.at[q], core_peer)
        for q, at in enumerate(columns)
    ]
    over_y = []
    for q, at in enumerate(columns):
        over_core[q].wait_recv()
        core_sum[:, :, :, at] = part_ref[:, :, c, :, at] + core_in[:, :, :, at]
        over_y.append(
            send(core_sum.at[:, 1 - y, :, at], y_in.at[:, :, at], y_s.at[q], y_r.at[q], y_peer)
        )
    over_z = []
    for q, at in enumerate(columns):
        over_y[q].wait_recv()
        y_sum[:, :, at] = core_sum[:, y, :, at] + y_in[:, :, at]
        over_z.append([
            send(y_sum.at[spot, :, at], z_in.at[k, :, at], z_s.at[q, k], z_r.at[q, k], z_peers[k])
            for k, spot in enumerate(z_spots)
        ])
    give_z = []
    for q, at in enumerate(columns):
        total = y_sum[z, :, at] - target_ref[:, at].astype(jnp.float32)
        for k, copy in enumerate(over_z[q]):
            copy.wait_recv()
            total = total + z_in[k, :, at]
        out_ref[z, y, c, :, at] = jnp.tanh(total).astype(jnp.bfloat16)
        mine = out_ref.at[z, y, c, :, at]
        give_z.append([
            send(mine, mine, gz_s.at[q, k], gz_r.at[q, k], peer) for k, peer in enumerate(z_peers)
        ])
    give_y = []
    for q, at in enumerate(columns):
        for copy in give_z[q]:
            copy.wait_recv()
        mine = out_ref.at[:, y, c, :, at]
        give_y.append(send(mine, mine, gy_s.at[q], gy_r.at[q], y_peer))
    give_core = []
    for q, at in enumerate(columns):
        give_y[q].wait_recv()
        mine = out_ref.at[:, :, c, :, at]
        give_core.append(send(mine, mine, gc_s.at[q], gc_r.at[q], core_peer))
    for copy in give_core:
        copy.wait_recv()
    if lends is not None:
        for j in range(z_size):
            pl.when(helps[j] if lends else home)(lambda j=j: relay(j).wait_recv())
        relay_all(lambda j: relay(j).wait_send())
    for copy in [*over_core, *over_y, *sum(over_z, []), *sum(give_z, []), *give_y, *give_core]:
        copy.wait_send()


def residual(output, own_target, n, which, lends=None, near=None):
    tokens, width = output.shape
    share, z_size = tokens // n, n // 4
    one = pltpu.SemaphoreType.DMA((PIECES,))
    many = pltpu.SemaphoreType.DMA((PIECES, z_size - 1))
    there = pl.BlockSpec(memory_space=pltpu.VMEM)
    shapes = [jax.ShapeDtypeStruct((z_size, 2, 2, share, width), jnp.bfloat16)]
    operands = [output.reshape(z_size, 2, 2, share, width), own_target]
    if lends is not None:
        operands.append(near)
        wide = width // z_size if lends else width
        shapes.append(jax.ShapeDtypeStruct((near.shape[0], wide), near.dtype))
    resid, *far = pl.pallas_call(
        functools.partial(residual_kernel, z_size, lends),
        out_shape=shapes,
        in_specs=[there] * len(operands),
        out_specs=[there] * len(shapes),
        scratch_shapes=[
            pltpu.VMEM((z_size, 2, share, width), jnp.float32),
            pltpu.VMEM((z_size, 2, share, width), jnp.float32),
            pltpu.VMEM((z_size, share, width), jnp.float32),
            pltpu.VMEM((z_size, share, width), jnp.float32),
            pltpu.VMEM((z_size - 1, share, width), jnp.float32),
            one, one, one, one, many, many, many, many, one, one, one, one,
            *([] if lends is None else [pltpu.SemaphoreType.DMA((z_size,))] * 2),
        ],
        compiler_params=pltpu.CompilerParams(collective_id=which, has_side_effects=True),
        cost_estimate=pl.CostEstimate(flops=0, bytes_accessed=100 * tokens * width, transcendentals=0),
        name="residual",
    )(*operands)
    return (resid.reshape(tokens, width), *far)


def add_kernel(count, weights_ref, base_ref, *refs):
    out_ref = refs[-1]
    total = base_ref[...]
    for i, other in enumerate(refs[:count]):
        total = total + weights_ref[i] * other[...].astype(jnp.float32)
    out_ref[...] = total.astype(out_ref.dtype)


def add_others(base, others, weights, block):
    rows, width = base.shape
    count = others[0].shape[0] // block
    here = pl.BlockSpec((block, width), lambda i: (i, 0))
    return pl.pallas_call(
        functools.partial(add_kernel, len(others)),
        grid=(count,),
        out_shape=jax.ShapeDtypeStruct((rows, width), jnp.bfloat16),
        in_specs=[pl.BlockSpec(memory_space=pltpu.SMEM), here] + [here] * len(others),
        out_specs=here,
        compiler_params=pltpu.CompilerParams(dimension_semantics=("arbitrary",)),
        cost_estimate=pl.CostEstimate(
            flops=4 * count * block * width, bytes_accessed=8 * count * block * width, transcendentals=0
        ),
        name="add_others",
    )(weights, base, *others)


def step(params, tracker, hidden, target):
    groups, n = lax.axis_size("grp"), lax.axis_size("blk")
    weights = mix_weights(lax.axis_index("grp"), groups)
    tokens = hidden.shape[0]
    share = tokens // n
    own_target = lax.dynamic_slice_in_dim(target, lax.axis_index("blk") * share, share, 0)
    params, tracker = params[0], tracker[0]
    rows = params.shape[0]
    block = 16
    first = rows * 5 // 7 // 16 * 16
    ends = sorted({first, max(first, rows - 40), max(first, rows - 16), rows})
    cuts = list(zip([0, *ends[:-1]], ends))
    other_params = exchange(params, groups)
    slices = [tracker[lo:hi] for lo, hi in cuts]
    output_old = jnp.dot(hidden, params, preferred_element_type=jnp.float32)
    relayed = groups == 2 and n >= 8
    if relayed:
        resid_old, lent = residual(output_old, own_target, n, 0, True, slices[-1])
        both, spots = ("grp", "blk"), helpers(n // 4)
        carried = lax.ppermute(lent, both, [(n + spot, spot) for spot in spots])
    else:
        (resid_old,) = residual(output_old, own_target, n, 0)
    other_tracker = []
    for piece in slices[:-1]:
        other_tracker.append(exchange(piece, groups))
    params_next = (
        mixed(params, other_params, weights) - step_size * tracker.astype(jnp.float32)
    ).astype(jnp.bfloat16)
    output_new = jnp.dot(hidden, params_next, preferred_element_type=jnp.float32)
    if relayed:
        pairs = [(b, n + b) for b in range(n)] + [(n + b, b) for b in range(1, n)]
        last = {(-1, 1): lax.ppermute(slices[-1], both, pairs)}
    else:
        last = exchange(slices[-1], groups)
    if relayed:
        resid_new, returned = residual(output_new, own_target, n, 1, False, carried)
        last = {key: value + returned for key, value in last.items()}
    else:
        (resid_new,) = residual(output_new, own_target, n, 1)
    other_tracker.append(last)
    change = lax.dot_general(
        jnp.concatenate([hidden, -hidden], 0),
        jnp.concatenate([resid_new, resid_old], 0),
        (((0,), (0,)), ((), ())),
        preferred_element_type=jnp.float32,
    )
    base = weights[0] * tracker.astype(jnp.float32) + change / tokens
    late = lax.optimization_barrier([base[lo:hi] for lo, hi in cuts[1:]])
    gains = jnp.stack([sum(weights[o] for o in offsets) for offsets in other_tracker[0]])
    early = list(other_tracker[0].values())
    height = next(size for size in (10 * block, 4 * block, block) if first % size == 0)
    tracker_next = add_others(base, early, gains, height)
    for (lo, _), piece, received in zip(cuts[1:], late, other_tracker[1:]):
        for gain, value in zip(gains, received.values()):
            piece = piece + gain * value.astype(jnp.float32)
        tracker_next = lax.dynamic_update_slice(tracker_next, piece.astype(jnp.bfloat16), (lo, 0))
    return (params_next[None], tracker_next[None])


def solution(mesh):
    placed = (P("grp", "blk", None), P("grp", "blk", None), P("grp", "blk"), P("grp", None))
    return jax.shard_map(
        step,
        mesh=mesh,
        in_specs=placed,
        out_specs=(P("grp", "blk", None), P("grp", "blk", None)),
        check_vma=False,
    )
```

```python
import functools

import jax
import jax.numpy as jnp
from jax import lax
from jax.experimental import pallas as pl
from jax.experimental.pallas import tpu as pltpu
from jax.sharding import PartitionSpec as P


step_size = 0.05
MESH = pl.DeviceIdType.MESH


def mix_weights(position, groups):
    def has(spot):
        return ((spot >= 0) & (spot < groups)).astype(jnp.float32)

    def row(spot):
        a, b = has(spot - 1) / 3.0, has(spot + 1) / 3.0
        return a, 1.0 - a - b, b

    here, before, after = row(position), row(position - 1), row(position + 1)
    return {
        -2: here[0] * before[0],
        -1: here[0] * before[1] + here[1] * here[0],
        0: here[1] * here[1] + here[0] * before[2] + here[2] * after[0],
        1: here[2] * after[1] + here[1] * here[2],
        2: here[2] * after[2],
    }


def exchange(value, groups):
    if groups == 2:
        return {(-1, 1): lax.ppermute(value, "grp", [(0, 1), (1, 0)])}
    received = {}
    for offset in (-2, -1, 1, 2):
        pairs = [(i, i - offset) for i in range(groups) if 0 <= i - offset < groups]
        if pairs:
            received[(offset,)] = lax.ppermute(value, "grp", pairs)
    return received


def helpers(z_size):
    return [2 * chip + 1 for chip in range(2 * z_size)]


def mixed(own, others, weights):
    total = weights[0] * own.astype(jnp.float32)
    for offsets, value in others.items():
        total = total + sum(weights[o] for o in offsets) * value.astype(jnp.float32)
    return total


PIECES = 4


def residual_kernel(z_size, lends, part_ref, target_ref, *refs):
    if lends is not None:
        near_ref, *refs = refs
        home_ref, *refs = refs if not lends else [None, *refs]
        out_ref, far_ref, *refs = refs
    else:
        out_ref, *refs = refs
    core_in, core_sum, y_in, y_sum, z_in, *sems = refs
    (core_s, core_r, y_s, y_r, z_s, z_r, gz_s, gz_r, gy_s, gy_r, gc_s, gc_r) = sems[:12]
    me = lax.axis_index("blk")
    c = lax.rem(me, 2)
    y = lax.rem(lax.div(me, 2), 2)
    z = lax.div(me, 4)
    core_peer = z * 4 + y * 2 + (1 - c)
    y_peer = z * 4 + (1 - y) * 2 + c
    z_spots = [lax.rem(z + k, z_size) for k in range(1, z_size)]
    z_peers = [spot * 4 + y * 2 + c for spot in z_spots]
    width = target_ref.shape[-1] // PIECES
    columns = [pl.ds(q * width, width) for q in range(PIECES)]

    greeted = [core_peer, y_peer, *z_peers]
    if lends is not None:
        relay_s, relay_r = sems[12:]
        greeted += [spot * 4 + y * 2 + 1 - c for spot in z_spots]
        greeted += [spot * 4 + (1 - y) * 2 + 1 - c for spot in [z, *z_spots]]
        length = target_ref.shape[-1] // (2 * z_size)
        late_side = lax.axis_index("grp") == (1 if lends else 0)
        travels = [late_side | (j >= z_size) for j in range(2 * z_size)]
        homes = [(me == 0) & travel for travel in travels]
        helps = [(me == spot) & travel for spot, travel in zip(helpers(z_size), travels)]
        if lends:
            fills = [(functools.reduce(lambda a, b: a | b, helps), pl.ds(0, length))]
        else:
            fills = [(home, pl.ds(j * length, length)) for j, home in enumerate(homes)]
        for filled, at in fills:

            @pl.when(jnp.logical_not(filled))
            def _(at=at):
                if lends or at.start >= home_ref.shape[-1]:
                    far_ref[:, at] = jnp.zeros((far_ref.shape[0], length), far_ref.dtype)
                else:
                    far_ref[:, at] = home_ref[:, at]

    barrier = pltpu.get_barrier_semaphore()
    for peer in greeted:
        pl.semaphore_signal(barrier, inc=1, device_id={"blk": peer}, device_id_type=MESH)
    pl.semaphore_wait(barrier, len(greeted))

    def relay(j):
        at = pl.ds(j * length, length)
        return pltpu.make_async_remote_copy(
            src_ref=near_ref.at[:, at] if lends else near_ref,
            dst_ref=far_ref if lends else far_ref.at[:, at],
            send_sem=relay_s.at[j],
            recv_sem=relay_r.at[j],
            device_id={"blk": helpers(z_size)[j] if lends else 0},
            device_id_type=MESH,
        )

    def relay_all(act):
        for j in range(2 * z_size):
            pl.when(homes[j] if lends else helps[j])(functools.partial(act, j))

    if lends is not None:
        relay_all(lambda j: relay(j).start())

    def send(src, dst, send_sem, recv_sem, peer):
        copy = pltpu.make_async_remote_copy(
            src_ref=src,
            dst_ref=dst,
            send_sem=send_sem,
            recv_sem=recv_sem,
            device_id={"blk": peer},
            device_id_type=MESH,
        )
        copy.start()
        return copy

    over_core = [
        send(part_ref.at[:, :, 1 - c, :, at], core_in.at[:, :, :, at], core_s.at[q], core_r.at[q], core_peer)
        for q, at in enumerate(columns)
    ]
    over_y = []
    for q, at in enumerate(columns):
        over_core[q].wait_recv()
        core_sum[:, :, :, at] = part_ref[:, :, c, :, at] + core_in[:, :, :, at]
        over_y.append(
            send(core_sum.at[:, 1 - y, :, at], y_in.at[:, :, at], y_s.at[q], y_r.at[q], y_peer)
        )
    over_z = []
    for q, at in enumerate(columns):
        over_y[q].wait_recv()
        y_sum[:, :, at] = core_sum[:, y, :, at] + y_in[:, :, at]
        over_z.append([
            send(y_sum.at[spot, :, at], z_in.at[k, :, at], z_s.at[q, k], z_r.at[q, k], z_peers[k])
            for k, spot in enumerate(z_spots)
        ])
    give_z = []
    for q, at in enumerate(columns):
        total = y_sum[z, :, at] - target_ref[:, at].astype(jnp.float32)
        for k, copy in enumerate(over_z[q]):
            copy.wait_recv()
            total = total + z_in[k, :, at]
        out_ref[z, y, c, :, at] = jnp.tanh(total).astype(jnp.bfloat16)
        mine = out_ref.at[z, y, c, :, at]
        give_z.append([
            send(mine, mine, gz_s.at[q, k], gz_r.at[q, k], peer) for k, peer in enumerate(z_peers)
        ])
    give_y = []
    for q, at in enumerate(columns):
        for copy in give_z[q]:
            copy.wait_recv()
        mine = out_ref.at[:, y, c, :, at]
        give_y.append(send(mine, mine, gy_s.at[q], gy_r.at[q], y_peer))
    give_core = []
    for q, at in enumerate(columns):
        give_y[q].wait_recv()
        mine = out_ref.at[:, :, c, :, at]
        give_core.append(send(mine, mine, gc_s.at[q], gc_r.at[q], core_peer))
    for copy in give_core:
        copy.wait_recv()
    if lends is not None:
        for j in range(2 * z_size):
            pl.when(helps[j] if lends else homes[j])(lambda j=j: relay(j).wait_recv())
        relay_all(lambda j: relay(j).wait_send())
    for copy in [*over_core, *over_y, *sum(over_z, []), *sum(give_z, []), *give_y, *give_core]:
        copy.wait_send()


def residual(output, own_target, n, which, lends=None, *near):
    tokens, width = output.shape
    share, z_size = tokens // n, n // 4
    one = pltpu.SemaphoreType.DMA((PIECES,))
    many = pltpu.SemaphoreType.DMA((PIECES, z_size - 1))
    there = pl.BlockSpec(memory_space=pltpu.VMEM)
    shapes = [jax.ShapeDtypeStruct((z_size, 2, 2, share, width), jnp.bfloat16)]
    operands = [output.reshape(z_size, 2, 2, share, width), own_target]
    if lends is not None:
        operands += near
        wide = width // (2 * z_size) if lends else width
        shapes.append(jax.ShapeDtypeStruct((near[0].shape[0], wide), near[0].dtype))
    resid, *far = pl.pallas_call(
        functools.partial(residual_kernel, z_size, lends),
        out_shape=shapes,
        in_specs=[there] * len(operands),
        out_specs=[there] * len(shapes),
        scratch_shapes=[
            pltpu.VMEM((z_size, 2, share, width), jnp.float32),
            pltpu.VMEM((z_size, 2, share, width), jnp.float32),
            pltpu.VMEM((z_size, share, width), jnp.float32),
            pltpu.VMEM((z_size, share, width), jnp.float32),
            pltpu.VMEM((z_size - 1, share, width), jnp.float32),
            one, one, one, one, many, many, many, many, one, one, one, one,
            *([] if lends is None else [pltpu.SemaphoreType.DMA((2 * z_size,))] * 2),
        ],
        compiler_params=pltpu.CompilerParams(collective_id=which, has_side_effects=True),
        cost_estimate=pl.CostEstimate(flops=0, bytes_accessed=100 * tokens * width, transcendentals=0),
        name="residual",
    )(*operands)
    return (resid.reshape(tokens, width), *far)


def add_kernel(count, weights_ref, base_ref, *refs):
    out_ref = refs[-1]
    total = base_ref[...]
    for i, other in enumerate(refs[:count]):
        total = total + weights_ref[i] * other[...].astype(jnp.float32)
    out_ref[...] = total.astype(out_ref.dtype)


def add_others(base, others, weights, block):
    rows, width = base.shape
    count = others[0].shape[0] // block
    here = pl.BlockSpec((block, width), lambda i: (i, 0))
    return pl.pallas_call(
        functools.partial(add_kernel, len(others)),
        grid=(count,),
        out_shape=jax.ShapeDtypeStruct((rows, width), jnp.bfloat16),
        in_specs=[pl.BlockSpec(memory_space=pltpu.SMEM), here] + [here] * len(others),
        out_specs=here,
        compiler_params=pltpu.CompilerParams(dimension_semantics=("arbitrary",)),
        cost_estimate=pl.CostEstimate(
            flops=4 * count * block * width, bytes_accessed=8 * count * block * width, transcendentals=0
        ),
        name="add_others",
    )(weights, base, *others)


def step(params, tracker, hidden, target):
    groups, n = lax.axis_size("grp"), lax.axis_size("blk")
    weights = mix_weights(lax.axis_index("grp"), groups)
    tokens = hidden.shape[0]
    share = tokens // n
    own_target = lax.dynamic_slice_in_dim(target, lax.axis_index("blk") * share, share, 0)
    params, tracker = params[0], tracker[0]
    rows = params.shape[0]
    block = 16
    first = rows * 5 // 7 // 16 * 16
    ends = sorted({first, max(first, rows - 40), max(first, rows - 16), rows})
    cuts = list(zip([0, *ends[:-1]], ends))
    other_params = exchange(params, groups)
    slices = [tracker[lo:hi] for lo, hi in cuts]
    output_old = jnp.dot(hidden, params, preferred_element_type=jnp.float32)
    relayed = groups == 2 and n >= 8
    if relayed:
        resid_old, lent = residual(output_old, own_target, n, 0, True, slices[-1])
        both, spots = ("grp", "blk"), helpers(n // 4)
        inward = [(n + spot, spot) for spot in spots]
        outward = [(spot, n + spot) for spot in spots[len(spots) // 2 :]]
        width = params.shape[1]
        beside = lax.ppermute(slices[-1][:, : width // 2], both, [(0, 1)])
        home = lax.ppermute(beside, both, [(1, n)])
        carried = lax.ppermute(lent, both, outward + inward)
    else:
        (resid_old,) = residual(output_old, own_target, n, 0)
    other_tracker = []
    for piece in slices[:-1]:
        other_tracker.append(exchange(piece, groups))
    params_next = (
        mixed(params, other_params, weights) - step_size * tracker.astype(jnp.float32)
    ).astype(jnp.bfloat16)
    output_new = jnp.dot(hidden, params_next, preferred_element_type=jnp.float32)
    if relayed:
        pairs = [(g * n + b, (1 - g) * n + b) for g in range(2) for b in range(1, n)]
        last = {(-1, 1): lax.ppermute(slices[-1], both, pairs)}
    else:
        last = exchange(slices[-1], groups)
    if relayed:
        resid_new, returned = residual(output_new, own_target, n, 1, False, carried, home)
    else:
        (resid_new,) = residual(output_new, own_target, n, 1)
    other_tracker.append(last)
    change = lax.dot_general(
        jnp.concatenate([hidden, -hidden], 0),
        jnp.concatenate([resid_new, resid_old], 0),
        (((0,), (0,)), ((), ())),
        preferred_element_type=jnp.float32,
    )
    base = weights[0] * tracker.astype(jnp.float32) + change / tokens
    late = lax.optimization_barrier([base[lo:hi] for lo, hi in cuts[1:]])
    gains = jnp.stack([sum(weights[o] for o in offsets) for offsets in other_tracker[0]])
    if relayed:
        late[-1] = late[-1] + gains[0] * returned.astype(jnp.float32)
    early = list(other_tracker[0].values())
    height = next(size for size in (10 * block, 4 * block, block) if first % size == 0)
    tracker_next = add_others(base, early, gains, height)
    for (lo, _), piece, received in zip(cuts[1:], late, other_tracker[1:]):
        for gain, value in zip(gains, received.values()):
            piece = piece + gain * value.astype(jnp.float32)
        tracker_next = lax.dynamic_update_slice(tracker_next, piece.astype(jnp.bfloat16), (lo, 0))
    return (params_next[None], tracker_next[None])


def solution(mesh):
    placed = (P("grp", "blk", None), P("grp", "blk", None), P("grp", "blk"), P("grp", None))
    return jax.shard_map(
        step,
        mesh=mesh,
        in_specs=placed,
        out_specs=(P("grp", "blk", None), P("grp", "blk", None)),
        check_vma=False,
    )
```

```python
import functools

import jax
import jax.numpy as jnp
from jax import lax
from jax.experimental import pallas as pl
from jax.experimental.pallas import tpu as pltpu
from jax.sharding import PartitionSpec as P


step_size = 0.05
MESH = pl.DeviceIdType.MESH


def mix_weights(position, groups):
    def has(spot):
        return ((spot >= 0) & (spot < groups)).astype(jnp.float32)

    def row(spot):
        a, b = has(spot - 1) / 3.0, has(spot + 1) / 3.0
        return a, 1.0 - a - b, b

    here, before, after = row(position), row(position - 1), row(position + 1)
    return {
        -2: here[0] * before[0],
        -1: here[0] * before[1] + here[1] * here[0],
        0: here[1] * here[1] + here[0] * before[2] + here[2] * after[0],
        1: here[2] * after[1] + here[1] * here[2],
        2: here[2] * after[2],
    }


def exchange(value, groups):
    if groups == 2:
        return {(-1, 1): lax.ppermute(value, "grp", [(0, 1), (1, 0)])}
    received = {}
    for offset in (-2, -1, 1, 2):
        pairs = [(i, i - offset) for i in range(groups) if 0 <= i - offset < groups]
        if pairs:
            received[(offset,)] = lax.ppermute(value, "grp", pairs)
    return received


def helpers(z_size):
    return [2 * chip + 1 for chip in range(2 * z_size)]


def mixed(own, others, weights):
    total = weights[0] * own.astype(jnp.float32)
    for offsets, value in others.items():
        total = total + sum(weights[o] for o in offsets) * value.astype(jnp.float32)
    return total


PIECES = 4


def residual_kernel(z_size, lends, part_ref, target_ref, *refs):
    if lends is not None:
        near_ref, out_ref, far_ref, *refs = refs
    else:
        out_ref, *refs = refs
    core_in, core_sum, y_in, y_sum, z_in, *sems = refs
    (core_s, core_r, y_s, y_r, z_s, z_r, gz_s, gz_r, gy_s, gy_r, gc_s, gc_r) = sems[:12]
    me = lax.axis_index("blk")
    c = lax.rem(me, 2)
    y = lax.rem(lax.div(me, 2), 2)
    z = lax.div(me, 4)
    core_peer = z * 4 + y * 2 + (1 - c)
    y_peer = z * 4 + (1 - y) * 2 + c
    z_spots = [lax.rem(z + k, z_size) for k in range(1, z_size)]
    z_peers = [spot * 4 + y * 2 + c for spot in z_spots]
    width = target_ref.shape[-1] // PIECES
    columns = [pl.ds(q * width, width) for q in range(PIECES)]

    greeted = [core_peer, y_peer, *z_peers]
    if lends is not None:
        relay_s, relay_r = sems[12:]
        greeted += [spot * 4 + y * 2 + 1 - c for spot in z_spots]
        greeted += [spot * 4 + (1 - y) * 2 + 1 - c for spot in [z, *z_spots]]
        home = (lax.axis_index("grp") == (1 if lends else 0)) & (me == 0)
        helps = [
            (lax.axis_index("grp") == (1 if lends else 0)) & (me == spot) for spot in helpers(z_size)
        ]
        receives = functools.reduce(lambda a, b: a | b, helps) if lends else home

        @pl.when(jnp.logical_not(receives))
        def _():
            far_ref[...] = jnp.zeros_like(far_ref)

    barrier = pltpu.get_barrier_semaphore()
    for peer in greeted:
        pl.semaphore_signal(barrier, inc=1, device_id={"blk": peer}, device_id_type=MESH)
    pl.semaphore_wait(barrier, len(greeted))

    def relay(j):
        length = target_ref.shape[-1] // (2 * z_size)
        at = pl.ds(j * length, length)
        return pltpu.make_async_remote_copy(
            src_ref=near_ref.at[:, at] if lends else near_ref,
            dst_ref=far_ref if lends else far_ref.at[:, at],
            send_sem=relay_s.at[j],
            recv_sem=relay_r.at[j],
            device_id={"blk": helpers(z_size)[j] if lends else 0},
            device_id_type=MESH,
        )

    def relay_all(act):
        for j in range(2 * z_size):
            pl.when(home if lends else helps[j])(functools.partial(act, j))

    if lends is not None:
        relay_all(lambda j: relay(j).start())

    def send(src, dst, send_sem, recv_sem, peer):
        copy = pltpu.make_async_remote_copy(
            src_ref=src,
            dst_ref=dst,
            send_sem=send_sem,
            recv_sem=recv_sem,
            device_id={"blk": peer},
            device_id_type=MESH,
        )
        copy.start()
        return copy

    over_core = [
        send(part_ref.at[:, :, 1 - c, :, at], core_in.at[:, :, :, at], core_s.at[q], core_r.at[q], core_peer)
        for q, at in enumerate(columns)
    ]
    over_y = []
    for q, at in enumerate(columns):
        over_core[q].wait_recv()
        core_sum[:, :, :, at] = part_ref[:, :, c, :, at] + core_in[:, :, :, at]
        over_y.append(
            send(core_sum.at[:, 1 - y, :, at], y_in.at[:, :, at], y_s.at[q], y_r.at[q], y_peer)
        )
    over_z = []
    for q, at in enumerate(columns):
        over_y[q].wait_recv()
        y_sum[:, :, at] = core_sum[:, y, :, at] + y_in[:, :, at]
        over_z.append([
            send(y_sum.at[spot, :, at], z_in.at[k, :, at], z_s.at[q, k], z_r.at[q, k], z_peers[k])
            for k, spot in enumerate(z_spots)
        ])
    give_z = []
    for q, at in enumerate(columns):
        total = y_sum[z, :, at] - target_ref[:, at].astype(jnp.float32)
        for k, copy in enumerate(over_z[q]):
            copy.wait_recv()
            total = total + z_in[k, :, at]
        out_ref[z, y, c, :, at] = jnp.tanh(total).astype(jnp.bfloat16)
        mine = out_ref.at[z, y, c, :, at]
        give_z.append([
            send(mine, mine, gz_s.at[q, k], gz_r.at[q, k], peer) for k, peer in enumerate(z_peers)
        ])
    give_y = []
    for q, at in enumerate(columns):
        for copy in give_z[q]:
            copy.wait_recv()
        mine = out_ref.at[:, y, c, :, at]
        give_y.append(send(mine, mine, gy_s.at[q], gy_r.at[q], y_peer))
    give_core = []
    for q, at in enumerate(columns):
        give_y[q].wait_recv()
        mine = out_ref.at[:, :, c, :, at]
        give_core.append(send(mine, mine, gc_s.at[q], gc_r.at[q], core_peer))
    for copy in give_core:
        copy.wait_recv()
    if lends is not None:
        for j in range(2 * z_size):
            pl.when(helps[j] if lends else home)(lambda j=j: relay(j).wait_recv())
        relay_all(lambda j: relay(j).wait_send())
    for copy in [*over_core, *over_y, *sum(over_z, []), *sum(give_z, []), *give_y, *give_core]:
        copy.wait_send()


def residual(output, own_target, n, which, lends=None, near=None):
    tokens, width = output.shape
    share, z_size = tokens // n, n // 4
    one = pltpu.SemaphoreType.DMA((PIECES,))
    many = pltpu.SemaphoreType.DMA((PIECES, z_size - 1))
    there = pl.BlockSpec(memory_space=pltpu.VMEM)
    shapes = [jax.ShapeDtypeStruct((z_size, 2, 2, share, width), jnp.bfloat16)]
    operands = [output.reshape(z_size, 2, 2, share, width), own_target]
    if lends is not None:
        operands.append(near)
        wide = width // (2 * z_size) if lends else width
        shapes.append(jax.ShapeDtypeStruct((near.shape[0], wide), near.dtype))
    resid, *far = pl.pallas_call(
        functools.partial(residual_kernel, z_size, lends),
        out_shape=shapes,
        in_specs=[there] * len(operands),
        out_specs=[there] * len(shapes),
        scratch_shapes=[
            pltpu.VMEM((z_size, 2, share, width), jnp.float32),
            pltpu.VMEM((z_size, 2, share, width), jnp.float32),
            pltpu.VMEM((z_size, share, width), jnp.float32),
            pltpu.VMEM((z_size, share, width), jnp.float32),
            pltpu.VMEM((z_size - 1, share, width), jnp.float32),
            one, one, one, one, many, many, many, many, one, one, one, one,
            *([] if lends is None else [pltpu.SemaphoreType.DMA((2 * z_size,))] * 2),
        ],
        compiler_params=pltpu.CompilerParams(collective_id=which, has_side_effects=True),
        cost_estimate=pl.CostEstimate(flops=0, bytes_accessed=100 * tokens * width, transcendentals=0),
        name="residual",
    )(*operands)
    return (resid.reshape(tokens, width), *far)


def add_kernel(count, weights_ref, base_ref, *refs):
    out_ref = refs[-1]
    total = base_ref[...]
    for i, other in enumerate(refs[:count]):
        total = total + weights_ref[i] * other[...].astype(jnp.float32)
    out_ref[...] = total.astype(out_ref.dtype)


def add_others(base, others, weights, block):
    rows, width = base.shape
    count = others[0].shape[0] // block
    here = pl.BlockSpec((block, width), lambda i: (i, 0))
    return pl.pallas_call(
        functools.partial(add_kernel, len(others)),
        grid=(count,),
        out_shape=jax.ShapeDtypeStruct((rows, width), jnp.bfloat16),
        in_specs=[pl.BlockSpec(memory_space=pltpu.SMEM), here] + [here] * len(others),
        out_specs=here,
        compiler_params=pltpu.CompilerParams(dimension_semantics=("arbitrary",)),
        cost_estimate=pl.CostEstimate(
            flops=4 * count * block * width, bytes_accessed=8 * count * block * width, transcendentals=0
        ),
        name="add_others",
    )(weights, base, *others)


def step(params, tracker, hidden, target):
    groups, n = lax.axis_size("grp"), lax.axis_size("blk")
    weights = mix_weights(lax.axis_index("grp"), groups)
    tokens = hidden.shape[0]
    share = tokens // n
    own_target = lax.dynamic_slice_in_dim(target, lax.axis_index("blk") * share, share, 0)
    params, tracker = params[0], tracker[0]
    rows = params.shape[0]
    block = 16
    first = rows * 6 // 7 // 16 * 16
    ends = sorted({first, max(first, rows - 16), rows})
    cuts = list(zip([0, *ends[:-1]], ends))
    other_params = exchange(params, groups)
    slices = [tracker[lo:hi] for lo, hi in cuts]
    output_old = jnp.dot(hidden, params, preferred_element_type=jnp.float32)
    relayed = groups == 2 and n >= 8
    if relayed:
        resid_old, lent = residual(output_old, own_target, n, 0, True, slices[-1])
        both, spots = ("grp", "blk"), helpers(n // 4)
        beside = lax.ppermute(slices[-1], both, [(0, 1)])
        home = lax.ppermute(beside, both, [(1, n)])
        carried = lax.ppermute(lent, both, [(n + spot, spot) for spot in spots])
    else:
        (resid_old,) = residual(output_old, own_target, n, 0)
    other_tracker = []
    for piece in slices[:-1]:
        other_tracker.append(exchange(piece, groups))
    params_next = (
        mixed(params, other_params, weights) - step_size * tracker.astype(jnp.float32)
    ).astype(jnp.bfloat16)
    output_new = jnp.dot(hidden, params_next, preferred_element_type=jnp.float32)
    if relayed:
        pairs = [(g * n + b, (1 - g) * n + b) for g in range(2) for b in range(1, n)]
        last = {(-1, 1): lax.ppermute(slices[-1], both, pairs)}
    else:
        last = exchange(slices[-1], groups)
    if relayed:
        resid_new, returned = residual(output_new, own_target, n, 1, False, carried)
    else:
        (resid_new,) = residual(output_new, own_target, n, 1)
    other_tracker.append(last)
    change = lax.dot_general(
        jnp.concatenate([hidden, -hidden], 0),
        jnp.concatenate([resid_new, resid_old], 0),
        (((0,), (0,)), ((), ())),
        preferred_element_type=jnp.float32,
    )
    base = weights[0] * tracker.astype(jnp.float32) + change / tokens
    late = lax.optimization_barrier([base[lo:hi] for lo, hi in cuts[1:]])
    gains = jnp.stack([sum(weights[o] for o in offsets) for offsets in other_tracker[0]])
    if relayed:
        late[-1] = late[-1] + gains[0] * (home + returned).astype(jnp.float32)
    early = list(other_tracker[0].values())
    height = next(size for size in (10 * block, 4 * block, block) if first % size == 0)
    tracker_next = add_others(base, early, gains, height)
    for (lo, _), piece, received in zip(cuts[1:], late, other_tracker[1:]):
        for gain, value in zip(gains, received.values()):
            piece = piece + gain * value.astype(jnp.float32)
        tracker_next = lax.dynamic_update_slice(tracker_next, piece.astype(jnp.bfloat16), (lo, 0))
    return (params_next[None], tracker_next[None])


def solution(mesh):
    placed = (P("grp", "blk", None), P("grp", "blk", None), P("grp", "blk"), P("grp", None))
    return jax.shard_map(
        step,
        mesh=mesh,
        in_specs=placed,
        out_specs=(P("grp", "blk", None), P("grp", "blk", None)),
        check_vma=False,
    )
```

```python
import functools

import jax
import jax.numpy as jnp
from jax import lax
from jax.experimental import pallas as pl
from jax.experimental.pallas import tpu as pltpu
from jax.sharding import PartitionSpec as P


step_size = 0.05
MESH = pl.DeviceIdType.MESH


def mix_weights(position, groups):
    def has(spot):
        return ((spot >= 0) & (spot < groups)).astype(jnp.float32)

    def row(spot):
        a, b = has(spot - 1) / 3.0, has(spot + 1) / 3.0
        return a, 1.0 - a - b, b

    here, before, after = row(position), row(position - 1), row(position + 1)
    return {
        -2: here[0] * before[0],
        -1: here[0] * before[1] + here[1] * here[0],
        0: here[1] * here[1] + here[0] * before[2] + here[2] * after[0],
        1: here[2] * after[1] + here[1] * here[2],
        2: here[2] * after[2],
    }


def exchange(value, groups):
    if groups == 2:
        return {(-1, 1): lax.ppermute(value, "grp", [(0, 1), (1, 0)])}
    received = {}
    for offset in (-2, -1, 1, 2):
        pairs = [(i, i - offset) for i in range(groups) if 0 <= i - offset < groups]
        if pairs:
            received[(offset,)] = lax.ppermute(value, "grp", pairs)
    return received


def helpers(z_size):
    return [2 * chip + 1 for chip in range(2 * z_size)]


def mixed(own, others, weights):
    total = weights[0] * own.astype(jnp.float32)
    for offsets, value in others.items():
        total = total + sum(weights[o] for o in offsets) * value.astype(jnp.float32)
    return total


PIECES = 4


def residual_kernel(z_size, lends, part_ref, target_ref, *refs):
    if lends is not None:
        near_ref, *refs = refs
        home_ref, *refs = refs if not lends else [None, *refs]
        out_ref, far_ref, *refs = refs
    else:
        out_ref, *refs = refs
    core_in, core_sum, y_in, y_sum, z_in, *sems = refs
    (core_s, core_r, y_s, y_r, z_s, z_r, gz_s, gz_r, gy_s, gy_r, gc_s, gc_r) = sems[:12]
    me = lax.axis_index("blk")
    c = lax.rem(me, 2)
    y = lax.rem(lax.div(me, 2), 2)
    z = lax.div(me, 4)
    core_peer = z * 4 + y * 2 + (1 - c)
    y_peer = z * 4 + (1 - y) * 2 + c
    z_spots = [lax.rem(z + k, z_size) for k in range(1, z_size)]
    z_peers = [spot * 4 + y * 2 + c for spot in z_spots]
    width = target_ref.shape[-1] // PIECES
    columns = [pl.ds(q * width, width) for q in range(PIECES)]

    greeted = [core_peer, y_peer, *z_peers]
    if lends is not None:
        relay_s, relay_r = sems[12:]
        greeted += [spot * 4 + y * 2 + 1 - c for spot in z_spots]
        greeted += [spot * 4 + (1 - y) * 2 + 1 - c for spot in [z, *z_spots]]
        length = target_ref.shape[-1] // (2 * z_size)
        late_side = lax.axis_index("grp") == (1 if lends else 0)
        travels = [late_side for _ in range(2 * z_size)]
        homes = [(me == 0) & travel for travel in travels]
        helps = [(me == spot) & travel for spot, travel in zip(helpers(z_size), travels)]
        if lends:
            fills = [(functools.reduce(lambda a, b: a | b, helps), pl.ds(0, length))]
        else:
            fills = [(home, pl.ds(j * length, length)) for j, home in enumerate(homes)]
        for filled, at in fills:

            @pl.when(jnp.logical_not(filled))
            def _(at=at):
                if lends:
                    far_ref[:, at] = jnp.zeros((far_ref.shape[0], length), far_ref.dtype)
                else:
                    far_ref[:, at] = home_ref[:, at]

    barrier = pltpu.get_barrier_semaphore()
    for peer in greeted:
        pl.semaphore_signal(barrier, inc=1, device_id={"blk": peer}, device_id_type=MESH)
    pl.semaphore_wait(barrier, len(greeted))

    def relay(j):
        at = pl.ds(j * length, length)
        return pltpu.make_async_remote_copy(
            src_ref=near_ref.at[:, at] if lends else near_ref,
            dst_ref=far_ref if lends else far_ref.at[:, at],
            send_sem=relay_s.at[j],
            recv_sem=relay_r.at[j],
            device_id={"blk": helpers(z_size)[j] if lends else 0},
            device_id_type=MESH,
        )

    def relay_all(act):
        for j in range(2 * z_size):
            pl.when(homes[j] if lends else helps[j])(functools.partial(act, j))

    if lends is not None:
        relay_all(lambda j: relay(j).start())

    def send(src, dst, send_sem, recv_sem, peer):
        copy = pltpu.make_async_remote_copy(
            src_ref=src,
            dst_ref=dst,
            send_sem=send_sem,
            recv_sem=recv_sem,
            device_id={"blk": peer},
            device_id_type=MESH,
        )
        copy.start()
        return copy

    over_core = [
        send(part_ref.at[:, :, 1 - c, :, at], core_in.at[:, :, :, at], core_s.at[q], core_r.at[q], core_peer)
        for q, at in enumerate(columns)
    ]
    over_y = []
    for q, at in enumerate(columns):
        over_core[q].wait_recv()
        core_sum[:, :, :, at] = part_ref[:, :, c, :, at] + core_in[:, :, :, at]
        over_y.append(
            send(core_sum.at[:, 1 - y, :, at], y_in.at[:, :, at], y_s.at[q], y_r.at[q], y_peer)
        )
    over_z = []
    for q, at in enumerate(columns):
        over_y[q].wait_recv()
        y_sum[:, :, at] = core_sum[:, y, :, at] + y_in[:, :, at]
        over_z.append([
            send(y_sum.at[spot, :, at], z_in.at[k, :, at], z_s.at[q, k], z_r.at[q, k], z_peers[k])
            for k, spot in enumerate(z_spots)
        ])
    give_z = []
    for q, at in enumerate(columns):
        total = y_sum[z, :, at] - target_ref[:, at].astype(jnp.float32)
        for k, copy in enumerate(over_z[q]):
            copy.wait_recv()
            total = total + z_in[k, :, at]
        out_ref[z, y, c, :, at] = jnp.tanh(total).astype(jnp.bfloat16)
        mine = out_ref.at[z, y, c, :, at]
        give_z.append([
            send(mine, mine, gz_s.at[q, k], gz_r.at[q, k], peer) for k, peer in enumerate(z_peers)
        ])
    give_y = []
    for q, at in enumerate(columns):
        for copy in give_z[q]:
            copy.wait_recv()
        mine = out_ref.at[:, y, c, :, at]
        give_y.append(send(mine, mine, gy_s.at[q], gy_r.at[q], y_peer))
    give_core = []
    for q, at in enumerate(columns):
        give_y[q].wait_recv()
        mine = out_ref.at[:, :, c, :, at]
        give_core.append(send(mine, mine, gc_s.at[q], gc_r.at[q], core_peer))
    for copy in give_core:
        copy.wait_recv()
    if lends is not None:
        for j in range(2 * z_size):
            pl.when(helps[j] if lends else homes[j])(lambda j=j: relay(j).wait_recv())
        relay_all(lambda j: relay(j).wait_send())
    for copy in [*over_core, *over_y, *sum(over_z, []), *sum(give_z, []), *give_y, *give_core]:
        copy.wait_send()


def residual(output, own_target, n, which, lends=None, *near):
    tokens, width = output.shape
    share, z_size = tokens // n, n // 4
    one = pltpu.SemaphoreType.DMA((PIECES,))
    many = pltpu.SemaphoreType.DMA((PIECES, z_size - 1))
    there = pl.BlockSpec(memory_space=pltpu.VMEM)
    shapes = [jax.ShapeDtypeStruct((z_size, 2, 2, share, width), jnp.bfloat16)]
    operands = [output.reshape(z_size, 2, 2, share, width), own_target]
    if lends is not None:
        operands += near
        wide = width // (2 * z_size) if lends else width
        shapes.append(jax.ShapeDtypeStruct((near[0].shape[0], wide), near[0].dtype))
    resid, *far = pl.pallas_call(
        functools.partial(residual_kernel, z_size, lends),
        out_shape=shapes,
        in_specs=[there] * len(operands),
        out_specs=[there] * len(shapes),
        scratch_shapes=[
            pltpu.VMEM((z_size, 2, share, width), jnp.float32),
            pltpu.VMEM((z_size, 2, share, width), jnp.float32),
            pltpu.VMEM((z_size, share, width), jnp.float32),
            pltpu.VMEM((z_size, share, width), jnp.float32),
            pltpu.VMEM((z_size - 1, share, width), jnp.float32),
            one, one, one, one, many, many, many, many, one, one, one, one,
            *([] if lends is None else [pltpu.SemaphoreType.DMA((2 * z_size,))] * 2),
        ],
        compiler_params=pltpu.CompilerParams(collective_id=which, has_side_effects=True),
        cost_estimate=pl.CostEstimate(flops=0, bytes_accessed=100 * tokens * width, transcendentals=0),
        name="residual",
    )(*operands)
    return (resid.reshape(tokens, width), *far)


def add_kernel(count, weights_ref, base_ref, *refs):
    out_ref = refs[-1]
    total = base_ref[...]
    for i, other in enumerate(refs[:count]):
        total = total + weights_ref[i] * other[...].astype(jnp.float32)
    out_ref[...] = total.astype(out_ref.dtype)


def add_others(base, others, weights, block):
    rows, width = base.shape
    count = others[0].shape[0] // block
    here = pl.BlockSpec((block, width), lambda i: (i, 0))
    return pl.pallas_call(
        functools.partial(add_kernel, len(others)),
        grid=(count,),
        out_shape=jax.ShapeDtypeStruct((rows, width), jnp.bfloat16),
        in_specs=[pl.BlockSpec(memory_space=pltpu.SMEM), here] + [here] * len(others),
        out_specs=here,
        compiler_params=pltpu.CompilerParams(dimension_semantics=("arbitrary",)),
        cost_estimate=pl.CostEstimate(
            flops=4 * count * block * width, bytes_accessed=8 * count * block * width, transcendentals=0
        ),
        name="add_others",
    )(weights, base, *others)


def step(params, tracker, hidden, target):
    groups, n = lax.axis_size("grp"), lax.axis_size("blk")
    weights = mix_weights(lax.axis_index("grp"), groups)
    tokens = hidden.shape[0]
    share = tokens // n
    own_target = lax.dynamic_slice_in_dim(target, lax.axis_index("blk") * share, share, 0)
    params, tracker = params[0], tracker[0]
    rows = params.shape[0]
    block = 16
    first = rows * 5 // 7 // 16 * 16
    ends = sorted({first, max(first, rows - 40), max(first, rows - 16), rows})
    cuts = list(zip([0, *ends[:-1]], ends))
    other_params = exchange(params, groups)
    slices = [tracker[lo:hi] for lo, hi in cuts]
    output_old = jnp.dot(hidden, params, preferred_element_type=jnp.float32)
    relayed = groups == 2 and n >= 8
    if relayed:
        resid_old, lent = residual(output_old, own_target, n, 0, True, slices[-1])
        both, spots = ("grp", "blk"), helpers(n // 4)
        inward = [(n + spot, spot) for spot in spots]
        beside = lax.ppermute(slices[-1], both, [(0, 1)])
        home = lax.ppermute(beside, both, [(1, n)])
        carried = lax.ppermute(lent, both, inward)
    else:
        (resid_old,) = residual(output_old, own_target, n, 0)
    other_tracker = []
    for piece in slices[:-1]:
        other_tracker.append(exchange(piece, groups))
    params_next = (
        mixed(params, other_params, weights) - step_size * tracker.astype(jnp.float32)
    ).astype(jnp.bfloat16)
    output_new = jnp.dot(hidden, params_next, preferred_element_type=jnp.float32)
    if relayed:
        pairs = [(g * n + b, (1 - g) * n + b) for g in range(2) for b in range(1, n)]
        last = {(-1, 1): lax.ppermute(slices[-1], both, pairs)}
    else:
        last = exchange(slices[-1], groups)
    if relayed:
        resid_new, returned = residual(output_new, own_target, n, 1, False, carried, home)
    else:
        (resid_new,) = residual(output_new, own_target, n, 1)
    other_tracker.append(last)
    change = lax.dot_general(
        jnp.concatenate([hidden, -hidden], 0),
        jnp.concatenate([resid_new, resid_old], 0),
        (((0,), (0,)), ((), ())),
        preferred_element_type=jnp.float32,
    )
    base = weights[0] * tracker.astype(jnp.float32) + change / tokens
    late = lax.optimization_barrier([base[lo:hi] for lo, hi in cuts[1:]])
    gains = jnp.stack([sum(weights[o] for o in offsets) for offsets in other_tracker[0]])
    if relayed:
        late[-1] = late[-1] + gains[0] * returned.astype(jnp.float32)
    early = list(other_tracker[0].values())
    height = next(size for size in (10 * block, 4 * block, block) if first % size == 0)
    tracker_next = add_others(base, early, gains, height)
    for (lo, _), piece, received in zip(cuts[1:], late, other_tracker[1:]):
        for gain, value in zip(gains, received.values()):
            piece = piece + gain * value.astype(jnp.float32)
        tracker_next = lax.dynamic_update_slice(tracker_next, piece.astype(jnp.bfloat16), (lo, 0))
    return (params_next[None], tracker_next[None])


def solution(mesh):
    placed = (P("grp", "blk", None), P("grp", "blk", None), P("grp", "blk"), P("grp", None))
    return jax.shard_map(
        step,
        mesh=mesh,
        in_specs=placed,
        out_specs=(P("grp", "blk", None), P("grp", "blk", None)),
        check_vma=False,
    )
```
